32 devices in a mesh: lat: 4 (over y, x), lon: 4 (over z), mem: 2 (over core).
Axes of the slice: x: 2, y: 2, z: 4, core: 2. Of those that a mesh axis runs over, the one named last changes fastest.
Arguments:
- anomalies: bfloat16 [24, 4, 1440, 512], P('mem', None, 'lon', 'lat'), may hold values from -6 to 6
- taper: float32 [4, 1440, 512], P('lon', 'lat'), may hold values from 0.5 to 8
- obs_row: int32 [256, 512], P('lat', 'lon'), may hold values from 0 to 511, as said below
- obs_col: int32 [256, 512], P('lat', 'lon'), may hold values from 0 to 1439, as said below
- obs_level: int32 [256, 512], P('lat', 'lon'), may hold values from 0 to 3
- obs_value: float32 [256, 512], P('lat', 'lon'), may hold values from -18 to 18
Outputs:
- increment: float32 [4, 1440, 512], P(None, 'lon', 'lat')
The draws below stay inside these ranges and needn't reach their ends.
Inputs may be any that keep to these rules, and one draw needn't show every extreme that they name: `obs_row`: the entry in row i lies in latitude rows (i // 64) * 128 to (i // 64 + 1) * 128 - 1, drawn evenly there. `obs_col`: the entry in column j lies in longitude columns (j // 128) * 360 to (j // 128 + 1) * 360 - 1, drawn evenly there.
All inputs are finite; a program needn't handle non-finite values.
Results may differ from the reference program's by a relative error of at most 0.0066.
Values may be sent and summed in bfloat16 or wider, within the bound.
A program may use at most 128 MiB of HBM per device.

```python
import math
import jax
import jax.numpy as jnp
from jax import lax

NLAT = 512
NLON = 1440
OBS_BLK = 64
L = 4
M = 24
ROWS_DEV = 128
COLS_DEV = 360
OBS_LAT = 256
OBS_LON = 512


def draw_obs_row(key, part):
    blocks = jnp.arange(OBS_LAT, dtype=jnp.int32)[:, None] // OBS_BLK
    offsets = jax.random.randint(jax.random.fold_in(key, 11), (OBS_LAT, OBS_LON), 0, ROWS_DEV, dtype=jnp.int32)
    return (blocks * ROWS_DEV + offsets).astype(jnp.int32)


def draw_obs_col(key, part):
    blocks = jnp.arange(OBS_LON, dtype=jnp.int32)[None, :] // 128
    offsets = jax.random.randint(jax.random.fold_in(key, 23), (OBS_LAT, OBS_LON), 0, COLS_DEV, dtype=jnp.int32)
    return (blocks * COLS_DEV + offsets).astype(jnp.int32)


def touch_ends(array, own_key, smallest, high):
    longest = array.shape.index(max(array.shape))
    spots = []
    for shift in (0, 1):
        where = [jax.random.randint(jax.random.fold_in(own_key, axis), (), 0, length) for axis, length in enumerate(array.shape)]
        where[longest] = (where[longest] + shift) % array.shape[longest]
        spots.append(tuple(where))
    return array.at[spots[0]].set(smallest).at[spots[1]].set(high)


def shard_levels(rng, extent, cuts, least, top_value):
    def one(dim, parts):
        heights = jax.random.uniform(jax.random.fold_in(jax.random.fold_in(rng, 6), dim), (parts,), jnp.float32, least / len(cuts), top_value / len(cuts))
        return jnp.repeat(jnp.exp(heights), extent[dim] // parts).reshape((-1,) + (1,) * (len(extent) - dim - 1))

    level = one(*cuts[0])
    for cut in cuts[1:]:
        level = level * one(*cut)
    return level


def centred(key, shape, spread, most, shards=(), held_as=jnp.bfloat16):
    level = shard_levels(key, shape, shards, -0.22, 0.18) if shards else 1.0
    entries = jax.random.normal(key, shape, jnp.float32) * spread * level
    return jnp.minimum(jnp.maximum(entries, -most), most).astype(held_as)


def setup_inputs(seed: int = 0) -> dict:
    streams_of = jax.random.split(jax.random.key(seed), 7)
    return {
        "anomalies": centred(streams_of[0], (M, L, NLON, NLAT), 1.0, 6.0, ((0, 2), (2, 4), (3, 4))),
        "taper": jnp.clip(jnp.exp(math.log(8.0) - 2.7725887 * jax.random.uniform(streams_of[1], (L, NLON, NLAT), jnp.float32) ** shard_levels(streams_of[1], (L, NLON, NLAT), ((0, 4), (1, 4)), -0.2, 0.2)), 0.5, 8.0),
        "obs_row": draw_obs_row(jax.random.fold_in(streams_of[6], 71), 0),
        "obs_col": draw_obs_col(jax.random.fold_in(streams_of[6], 71), 0),
        "obs_level": touch_ends(jax.random.randint(streams_of[4], (OBS_LAT, OBS_LON), 0, L), jax.random.fold_in(streams_of[4], 1), 0, L - 1).astype(jnp.int32),
        "obs_value": centred(streams_of[5], (OBS_LAT, OBS_LON), 3.0, 18.0, ((0, 4), (1, 4)), jnp.float32),
    }


def lon_basis(length):
    grid_idx = jnp.arange(length, dtype=jnp.int32)[:, None]
    coef_idx = jnp.arange(length, dtype=jnp.int32)[None, :]
    nyquist = length // 2
    wavenum = jnp.where(coef_idx <= nyquist, coef_idx, coef_idx - nyquist)
    phase_idx = grid_idx * wavenum % length
    angles = phase_idx.astype(jnp.float32) * (2.0 * math.pi / length)
    scales = jnp.where((coef_idx == 0) | (coef_idx == nyquist), 1.0 / math.sqrt(length), math.sqrt(2.0 / length))
    basis = jnp.where(coef_idx <= nyquist, jnp.cos(angles), jnp.sin(angles)) * scales
    return basis.astype(jnp.bfloat16)

def lat_basis(length):
    grid_idx = jnp.arange(length, dtype=jnp.int32)[:, None]
    mode_idx = jnp.arange(length, dtype=jnp.int32)[None, :]
    phase_idx = mode_idx * (2 * grid_idx + 1) % (4 * length)
    angles = phase_idx.astype(jnp.float32) * (math.pi / (2.0 * length))
    scales = jnp.where(mode_idx == 0, 1.0 / math.sqrt(length), math.sqrt(2.0 / length))
    return (jnp.cos(angles) * scales).astype(jnp.bfloat16)

def rounded(value):
    return lax.optimization_barrier(value.astype(jnp.bfloat16)).astype(jnp.float32)

def reference(anomalies, taper, obs_row, obs_col, obs_level, obs_value):
    innovation = jnp.zeros((L, NLON, NLAT), jnp.float32).at[obs_level, obs_col, obs_row].add(obs_value)
    innov_wide = rounded(innovation)
    lon_table = lon_basis(NLON).astype(jnp.float32)
    lat_table = lat_basis(NLAT).astype(jnp.float32)

    def accumulate(summed, member):
        member_wide = member.astype(jnp.float32)
        weighted = rounded(member_wide * innov_wide)
        zonal_coef = rounded(jnp.einsum('lxy,xk->lky', weighted, lon_table))
        spectrum = jnp.einsum('lky,yn->lkn', zonal_coef, lat_table)
        tapered = rounded(spectrum * taper)
        inverse = rounded(jnp.einsum('lkn,yn->lky', tapered, lat_table))
        localized = jnp.einsum('lky,xk->lxy', inverse, lon_table)
        return (summed + member_wide * localized, None)
    summed, _ = lax.scan(accumulate, jnp.zeros((L, NLON, NLAT), jnp.float32), anomalies)
    return summed / (M - 1)
```

```python
import math

import jax
import jax.numpy as jnp
from jax import lax
from jax.sharding import PartitionSpec as P

def lon_basis(length):
    nyquist = length // 2
    inner = next(size for size in range(32, 0, -1) if length % size == 0)
    outer = length // inner
    coef_idx = jnp.arange(length, dtype=jnp.int32)
    wavenum = jnp.where(coef_idx <= nyquist, coef_idx, coef_idx - nyquist)
    step = 2.0 * math.pi / length

    def angles(points):
        return (points[:, None] * wavenum[None, :] % length).astype(jnp.float32) * step

    coarse = angles(jnp.arange(outer, dtype=jnp.int32) * inner)
    fine = angles(jnp.arange(inner, dtype=jnp.int32))
    scales = jnp.where(
        (coef_idx == 0) | (coef_idx == nyquist), 1.0 / math.sqrt(length), math.sqrt(2.0 / length)
    )
    is_cos = (coef_idx <= nyquist)[None, :]
    coarse_cos, coarse_sin = jnp.cos(coarse) * scales, jnp.sin(coarse) * scales
    fine_cos, fine_sin = jnp.cos(fine), jnp.sin(fine)
    first = jnp.where(is_cos, coarse_cos, coarse_sin)
    second = jnp.where(is_cos, -coarse_sin, coarse_cos)
    first, second, fine_cos, fine_sin = lax.optimization_barrier((first, second, fine_cos, fine_sin))
    basis = first[:, None, :] * fine_cos[None] + second[:, None, :] * fine_sin[None]
    return basis.reshape(length, length).astype(jnp.bfloat16)


def lat_basis(length):
    grid_idx = jnp.arange(length, dtype=jnp.int32)[:, None]
    mode_idx = jnp.arange(length, dtype=jnp.int32)[None, :]
    phase_idx = mode_idx * (2 * grid_idx + 1) % (4 * length)
    angles = phase_idx.astype(jnp.float32) * (math.pi / (2.0 * length))
    scales = jnp.where(mode_idx == 0, 1.0 / math.sqrt(length), math.sqrt(2.0 / length))
    return (jnp.cos(angles) * scales).astype(jnp.bfloat16)


def spread_observations(cell_keys, row_local, obs_value, slot_count, row_count):
    obs_count = cell_keys.size
    block_rows = min(obs_count, 2048)
    turn_count = obs_count // block_rows
    key_blocks = cell_keys.reshape(turn_count, block_rows)
    row_blocks = row_local.reshape(turn_count, block_rows)
    value_blocks = obs_value.reshape(turn_count, block_rows)
    slot_ids = jnp.arange(slot_count, dtype=jnp.int32)
    row_ids = jnp.arange(row_count, dtype=jnp.int32)

    def add_block(running, obs_block):
        key_part, row_part, value_part = obs_block
        left_hot = (key_part[:, None] == slot_ids[None, :]).astype(jnp.bfloat16)
        high_part = value_part.astype(jnp.bfloat16)
        remainder = value_part - high_part.astype(jnp.float32)
        middle_part = remainder.astype(jnp.bfloat16)
        low_part = (remainder - middle_part.astype(jnp.float32)).astype(jnp.bfloat16)
        pieces = jnp.stack([high_part, middle_part, low_part], axis=1)
        row_hits = (row_part[:, None] == row_ids[None, :]).astype(jnp.bfloat16)
        weighted_rows = (pieces[:, :, None] * row_hits[:, None, :]).reshape(
            block_rows, 3 * row_count
        )
        added = jnp.einsum("ok,oz->kz", left_hot, weighted_rows, preferred_element_type=jnp.float32)
        return (running + added, None)

    start_sum = jnp.zeros((slot_count, 3 * row_count), jnp.float32)
    running, _ = lax.scan(add_block, start_sum, (key_blocks, row_blocks, value_blocks))
    return jnp.sum(running.reshape(slot_count, 3, row_count), axis=1)


def local(anomalies, taper, obs_row, obs_col, obs_level, obs_value):
    member_count, level_count, col_count, row_count = anomalies.shape
    lon_size, lat_size = lax.axis_size("lon"), lax.axis_size("lat")
    lon_total = col_count * lon_size
    lat_total = row_count * lat_size
    ensemble = member_count * lax.axis_size("mem")
    own_members = member_count // lat_size
    everyone = ("lat", "lon")
    grouped = anomalies.reshape(lat_size, own_members, lon_size, col_count, row_count)
    fields = [
        lax.all_to_all(
            grouped[:, turn].reshape(lat_size * lon_size, col_count, row_count),
            everyone, split_axis=0, concat_axis=0, tiled=True,
        )
        for turn in range(own_members)
    ]
    row_start = lax.axis_index("lat") * row_count
    col_start = lax.axis_index("lon") * col_count
    cell_keys = (obs_level * col_count + (obs_col - col_start)).reshape(-1)
    row_local = (obs_row - row_start).reshape(-1)
    innovation = spread_observations(
        cell_keys, row_local, obs_value.reshape(-1), level_count * col_count, row_count
    )
    innovation = innovation.reshape(level_count, col_count, row_count).astype(jnp.bfloat16)
    innov_cols = lax.all_to_all(innovation, "lon", split_axis=0, concat_axis=0, tiled=True)
    innov_all = lax.all_gather(innov_cols.reshape(lon_total, row_count), "lat")
    taper_all = lax.all_gather(
        taper[0].astype(jnp.bfloat16), "lat", axis=0, tiled=True
    ).astype(jnp.float32)
    lon_table = lon_basis(lon_total)
    lat_table = lat_basis(lat_total)
    total = jnp.zeros((lat_size, lon_total, row_count), jnp.float32)
    for turn in range(own_members):
        field = fields[turn].reshape(lat_size, lon_total, row_count)
        zonal = jnp.einsum(
            "ixy,xk->kiy", field * innov_all, lon_table, preferred_element_type=jnp.float32
        ).astype(jnp.bfloat16).reshape(lon_total, lat_total)
        spectrum = jnp.einsum("ky,yn->kn", zonal, lat_table, preferred_element_type=jnp.float32)
        tapered = (spectrum * taper_all).astype(jnp.bfloat16)
        inverse = jnp.einsum(
            "kn,yn->ky", tapered, lat_table, preferred_element_type=jnp.float32
        ).astype(jnp.bfloat16).reshape(lon_total, lat_size, row_count)
        localized = jnp.einsum("kiy,xk->ixy", inverse, lon_table, preferred_element_type=jnp.float32)
        total = total + field.astype(jnp.float32) * localized
    parts = lax.all_to_all(total.astype(jnp.bfloat16), "lat", split_axis=0, concat_axis=0, tiled=True)
    merged = lax.psum(jnp.sum(parts.astype(jnp.float32), axis=0), "mem")
    blocks = merged.reshape(lon_size, col_count, row_count) / (ensemble - 1)
    summed = lax.all_to_all(blocks.astype(jnp.bfloat16), "lon", split_axis=0, concat_axis=0, tiled=True)
    return summed.astype(jnp.float32)


def solution(mesh):
    in_specs = (
        P("mem", None, "lon", "lat"),
        P("lon", "lat", None),
        P("lat", "lon"),
        P("lat", "lon"),
        P("lat", "lon"),
        P("lat", "lon"),
    )
    out_specs = P(None, "lon", "lat")
    return jax.shard_map(local, mesh=mesh, in_specs=in_specs, out_specs=out_specs, check_vma=False)
```

```python
import functools
import math

import jax
import jax.numpy as jnp
from jax import lax
from jax.experimental import pallas as pl
from jax.experimental.pallas import tpu as pltpu
from jax.sharding import PartitionSpec as P

def lon_basis(length):
    nyquist = length // 2
    inner = next(size for size in range(32, 0, -1) if length % size == 0)
    outer = length // inner
    coef_idx = jnp.arange(length, dtype=jnp.int32)
    wavenum = jnp.where(coef_idx <= nyquist, coef_idx, coef_idx - nyquist)
    step = 2.0 * math.pi / length

    def angles(points):
        return (points[:, None] * wavenum[None, :] % length).astype(jnp.float32) * step

    coarse = angles(jnp.arange(outer, dtype=jnp.int32) * inner)
    fine = angles(jnp.arange(inner, dtype=jnp.int32))
    scales = jnp.where(
        (coef_idx == 0) | (coef_idx == nyquist), 1.0 / math.sqrt(length), math.sqrt(2.0 / length)
    )
    is_cos = (coef_idx <= nyquist)[None, :]
    coarse_cos, coarse_sin = jnp.cos(coarse) * scales, jnp.sin(coarse) * scales
    fine_cos, fine_sin = jnp.cos(fine), jnp.sin(fine)
    first = jnp.where(is_cos, coarse_cos, coarse_sin)
    second = jnp.where(is_cos, -coarse_sin, coarse_cos)
    first, second, fine_cos, fine_sin = lax.optimization_barrier((first, second, fine_cos, fine_sin))
    basis = first[:, None, :] * fine_cos[None] + second[:, None, :] * fine_sin[None]
    return basis.reshape(length, length).astype(jnp.bfloat16)


def lat_basis(length):
    grid_idx = jnp.arange(length, dtype=jnp.int32)[:, None]
    mode_idx = jnp.arange(length, dtype=jnp.int32)[None, :]
    phase_idx = mode_idx * (2 * grid_idx + 1) % (4 * length)
    angles = phase_idx.astype(jnp.float32) * (math.pi / (2.0 * length))
    scales = jnp.where(mode_idx == 0, 1.0 / math.sqrt(length), math.sqrt(2.0 / length))
    return (jnp.cos(angles) * scales).astype(jnp.bfloat16)


def fused_kernel(
    lat_size, lon_size, own, obs_rows,
    anom, taper, level, column, row, value, lon_fwd, lon_inv, lat_fwd, lat_inv, out,
    fields, table_fwd, table_inv, modes_fwd, modes_inv, taper_all, hits, innov_own, innov_all,
    weighted, inverse, total, partner_part, lat_send, lat_recv, lon_send, lon_recv,
    field_ss, field_rs, local_sem, table_sem, taper_ss, taper_rs, innov_ss, innov_rs,
    gather_ss, gather_rs, mem_sem, lat_ss, lat_rs, lon_ss, lon_rs, pair_sem,
):
    lat, lon, mem = lax.axis_index("lat"), lax.axis_index("lon"), lax.axis_index("mem")
    place_count = lat_size * lon_size
    half = lon_size // 2
    me = lat * lon_size + lon
    col_count, row_count = fields.shape[3:]
    f32, bf16 = jnp.float32, jnp.bfloat16

    def device(lat_idx, lon_idx, mem_idx):
        return {"lat": lat_idx, "lon": lon_idx, "mem": mem_idx}

    def place(offset):
        spot = lax.rem(me + offset, place_count)
        return lax.div(spot, lon_size), lax.rem(spot, lon_size)

    def remote(src, dst, send, recv, target):
        return pltpu.make_async_remote_copy(
            src_ref=src, dst_ref=dst, send_sem=send, recv_sem=recv,
            device_id=target, device_id_type=pl.DeviceIdType.MESH,
        )

    barrier = pltpu.get_barrier_semaphore()

    @pl.loop(1, place_count)
    def _(offset):
        lat_idx, lon_idx = place(offset)
        pl.semaphore_signal(
            barrier, inc=1, device_id=device(lat_idx, lon_idx, mem),
            device_id_type=pl.DeviceIdType.MESH,
        )

    pl.semaphore_signal(
        barrier, inc=1, device_id=device(lat, lon, 1 - mem),
        device_id_type=pl.DeviceIdType.MESH,
    )
    pl.semaphore_wait(barrier, place_count)

    def field_copy(turn, offset):
        lat_idx, lon_idx = place(offset)
        return remote(
            anom.at[lat_idx * own + turn, lon_idx], fields.at[turn, lat, lon],
            field_ss.at[turn, offset], field_rs.at[turn, offset], device(lat_idx, lon_idx, mem),
        )

    def send_fields(turn):
        @pl.loop(1, place_count)
        def _(offset):
            field_copy(turn, offset).start()

    def own_copy(turn):
        return pltpu.make_async_copy(
            anom.at[lat * own + turn, lon], fields.at[turn, lat, lon], local_sem.at[turn]
        )

    send_fields(0)
    taper_copies = [
        remote(
            taper, taper_all.at[lat], taper_ss.at[step], taper_rs.at[step],
            device(lax.rem(lat + step, lat_size), lon, mem),
        )
        for step in range(1, lat_size)
    ]
    table_copies = [
        pltpu.make_async_copy(src, dst, table_sem.at[idx])
        for idx, (src, dst) in enumerate([
            (lon_fwd, table_fwd), (lon_inv, table_inv), (lat_fwd, modes_fwd),
            (lat_inv, modes_inv), (taper, taper_all.at[lat]),
        ])
    ]
    for copy in table_copies:
        copy.start()
    for turn in range(own):
        own_copy(turn).start()

    hits[...] = jnp.zeros_like(hits)
    col_start, row_start = lon * col_count, lat * row_count
    group = 4

    @pl.loop(0, obs_rows // group)
    def _(step):
        def wide(ref):
            return jnp.concatenate([ref[pl.ds(step * group + part, 1), :] for part in range(group)], axis=1)

        keys = wide(level) * col_count + (wide(column) - col_start)
        local_row = wide(row) - row_start
        amount = wide(value)
        width = keys.shape[1]
        high = amount.astype(bf16).astype(f32)
        low = amount - high
        row_hot = lax.broadcasted_iota(jnp.int32, (row_count, width), 0) == local_row
        right = jnp.concatenate(
            [jnp.where(row_hot, high, 0.0).astype(bf16), jnp.where(row_hot, low, 0.0).astype(bf16)], axis=0
        )
        cells = lax.broadcasted_iota(jnp.int32, (col_count, width), 0)
        for lev in range(lon_size):
            left = jnp.where(cells == keys - lev * col_count, 1.0, 0.0).astype(bf16)
            hits[lev] += lax.dot_general(
                left, right, (((1,), (1,)), ((), ())), preferred_element_type=f32
            )

    for lev in range(lon_size):
        innov_own[lev] = (hits[lev, :, :row_count] + hits[lev, :, row_count:]).astype(bf16)
    innov_copies = [
        remote(
            innov_own.at[lax.rem(lon + step, lon_size)], innov_all.at[lat, lon],
            innov_ss.at[step], innov_rs.at[step], device(lat, lax.rem(lon + step, lon_size), mem),
        )
        for step in range(1, lon_size)
    ]
    for copy in innov_copies:
        copy.start()
    innov_local = pltpu.make_async_copy(innov_own.at[lon], innov_all.at[lat, lon], innov_ss.at[0])
    innov_local.start()
    for copy in taper_copies:
        copy.start()
    send_fields(1)
    innov_local.wait()
    for copy in innov_copies:
        copy.wait_recv()
    gather_copies = [
        remote(
            innov_all.at[lat], innov_all.at[lat], gather_ss.at[step], gather_rs.at[step],
            device(lax.rem(lat + step, lat_size), lon, mem),
        )
        for step in range(1, lat_size)
    ]
    for copy in gather_copies:
        copy.start()
    for turn in range(2, own):
        send_fields(turn)
    total[...] = jnp.zeros_like(total)
    for copy in table_copies:
        copy.wait()
    for copy in taper_copies + gather_copies:
        copy.wait_recv()

    @pl.loop(0, own)
    def _(turn):
        own_copy(turn).wait()

        @pl.loop(1, place_count)
        def _(offset):
            field_copy(turn, offset).wait_recv()

        @pl.loop(0, lon_size)
        def _(block):
            for band in range(lat_size):
                product = fields[turn, band, block].astype(f32) * innov_all[band, block].astype(f32)
                weighted[block, :, band * row_count:(band + 1) * row_count] = product.astype(bf16)

        @pl.loop(0, lat_size)
        def _(part):
            zonal = jnp.dot(table_fwd[0, part], weighted[0], preferred_element_type=f32)
            for block in range(1, lon_size):
                zonal += jnp.dot(table_fwd[block, part], weighted[block], preferred_element_type=f32)
            spectrum = jnp.dot(zonal.astype(bf16), modes_fwd[...], preferred_element_type=f32)
            tapered = (spectrum * taper_all[part].astype(f32)).astype(bf16)
            inverse[part] = jnp.dot(tapered, modes_inv[...], preferred_element_type=f32).astype(bf16)

        @pl.loop(0, lon_size)
        def _(block):
            localized = jnp.dot(table_inv[block, 0], inverse[0], preferred_element_type=f32)
            for part in range(1, lat_size):
                localized += jnp.dot(table_inv[block, part], inverse[part], preferred_element_type=f32)
            for band in range(lat_size):
                total[block, band] += (
                    fields[turn, band, block].astype(f32)
                    * localized[:, band * row_count:(band + 1) * row_count]
                )

    mem_copy = remote(
        total.at[pl.ds((1 - mem) * half, half)], partner_part, mem_sem.at[0], mem_sem.at[1],
        device(lat, lon, 1 - mem),
    )
    mem_copy.start()
    mem_copy.wait_recv()
    for block in range(half):
        for band in range(lat_size):
            lat_send[band, block] = (total[mem * half + block, band] + partner_part[block, band]).astype(bf16)
    lat_copies = [
        remote(
            lat_send.at[lax.rem(lat + step, lat_size)], lat_recv.at[step],
            lat_ss.at[step], lat_rs.at[step], device(lax.rem(lat + step, lat_size), lon, mem),
        )
        for step in range(1, lat_size)
    ]
    for copy in lat_copies:
        copy.start()
    for copy in lat_copies:
        copy.wait_recv()
    for block in range(half):
        summed = lat_send[lat, block].astype(f32)
        for step in range(1, lat_size):
            summed += lat_recv[step, block].astype(f32)
        lon_send[block] = summed.astype(bf16)

    def lon_copy(block):
        return remote(
            lon_send.at[block], lon_recv.at[lon], lon_ss.at[block], lon_rs.at[lon],
            device(lat, mem * half + block, mem),
        )

    def lon_local(block):
        return pltpu.make_async_copy(lon_send.at[block], lon_recv.at[lon], lon_ss.at[block])

    for block in range(half):
        pl.when(mem * half + block != lon)(lambda block=block: lon_copy(block).start())
        pl.when(mem * half + block == lon)(lambda block=block: lon_local(block).start())
    receives = lax.div(lon, half) == mem
    pair_copy = remote(lon_recv, lon_recv, pair_sem.at[0], pair_sem.at[1], device(lat, lon, 1 - mem))

    @pl.when(receives)
    def _():
        for step in range(1, lon_size):
            sender = lax.rem(lon + step, lon_size)
            remote(
                lon_send.at[0], lon_recv.at[sender], lon_ss.at[0], lon_rs.at[sender],
                device(lat, sender, mem),
            ).wait_recv()

    for block in range(half):
        pl.when(mem * half + block != lon)(lambda block=block: lon_copy(block).wait_send())
        pl.when(mem * half + block == lon)(lambda block=block: lon_local(block).wait())

    @pl.when(receives)
    def _():
        pair_copy.start()
        pair_copy.wait_send()

    @pl.when(jnp.logical_not(receives))
    def _():
        pair_copy.wait_recv()

    out[...] = lon_recv[...]
    mem_copy.wait_send()
    for copy in taper_copies + innov_copies + gather_copies + lat_copies:
        copy.wait_send()

    @pl.loop(0, own)
    def _(turn):
        @pl.loop(1, place_count)
        def _(offset):
            field_copy(turn, offset).wait_send()


def local(anomalies, taper, obs_row, obs_col, obs_level, obs_value):
    member_count, level_count, col_count, row_count = anomalies.shape
    lon_size, lat_size = lax.axis_size("lon"), lax.axis_size("lat")
    lon_total, lat_total = col_count * lon_size, row_count * lat_size
    ensemble = member_count * lax.axis_size("mem")
    own = member_count // lat_size
    place_count = lat_size * lon_size
    half = lon_size // 2
    part_count = taper.shape[1]
    lon_table = lon_basis(lon_total).reshape(lon_size, col_count, lat_size, part_count)
    lat_table = lat_basis(lat_total)
    f32, bf16 = jnp.float32, jnp.bfloat16
    slab = (col_count, row_count)
    whole = pl.BlockSpec(memory_space=pl.ANY)
    near = pl.BlockSpec(memory_space=pltpu.VMEM)
    dma = pltpu.SemaphoreType.DMA
    result = pl.pallas_call(
        functools.partial(fused_kernel, lat_size, lon_size, own, obs_row.shape[0]),
        out_shape=jax.ShapeDtypeStruct((level_count,) + slab, bf16),
        in_specs=[whole, whole, near, near, near, near, whole, whole, whole, whole],
        out_specs=near,
        scratch_shapes=[
            pltpu.VMEM((own, lat_size, lon_size) + slab, bf16),
            pltpu.VMEM((lon_size, lat_size, part_count, col_count), bf16),
            pltpu.VMEM((lon_size, lat_size, col_count, part_count), bf16),
            pltpu.VMEM((lat_total, lat_total), bf16),
            pltpu.VMEM((lat_total, lat_total), bf16),
            pltpu.VMEM((lat_size, part_count, lat_total), bf16),
            pltpu.VMEM((level_count, col_count, 2 * row_count), f32),
            pltpu.VMEM((level_count,) + slab, bf16),
            pltpu.VMEM((lat_size, lon_size) + slab, bf16),
            pltpu.VMEM((lon_size, col_count, lat_total), bf16),
            pltpu.VMEM((lat_size, part_count, lat_total), bf16),
            pltpu.VMEM((lon_size, lat_size) + slab, f32),
            pltpu.VMEM((half, lat_size) + slab, f32),
            pltpu.VMEM((lat_size, half) + slab, bf16),
            pltpu.VMEM((lat_size, half) + slab, bf16),
            pltpu.VMEM((half,) + slab, bf16),
            pltpu.VMEM((level_count,) + slab, bf16),
            dma((own, place_count)), dma((own, place_count)), dma((own,)), dma((5,)),
            dma((lat_size,)), dma((lat_size,)), dma((lon_size,)), dma((lon_size,)),
            dma((lat_size,)), dma((lat_size,)), dma((2,)), dma((lat_size,)), dma((lat_size,)),
            dma((half,)), dma((lon_size,)), dma((2,)),
        ],
        compiler_params=pltpu.CompilerParams(
            collective_id=0, has_side_effects=True, vmem_limit_bytes=60 * 1024 * 1024
        ),
    )(
        anomalies, taper[0].astype(bf16), obs_level, obs_col, obs_row, obs_value,
        lon_table.transpose(0, 2, 3, 1), lon_table.transpose(0, 2, 1, 3), lat_table, lat_table.T,
    )
    return result.astype(f32) / (ensemble - 1)


def solution(mesh):
    in_specs = (
        P("mem", None, "lon", "lat"),
        P("lon", "lat", None),
        P("lat", "lon"),
        P("lat", "lon"),
        P("lat", "lon"),
        P("lat", "lon"),
    )
    out_specs = P(None, "lon", "lat")
    return jax.shard_map(local, mesh=mesh, in_specs=in_specs, out_specs=out_specs, check_vma=False)
```

```python
import functools
import math

import jax
import jax.numpy as jnp
from jax import lax
from jax.experimental import pallas as pl
from jax.experimental.pallas import tpu as pltpu
from jax.sharding import PartitionSpec as P


def lon_factors(block_count, block_size, part_count, part_size):
    length = block_count * block_size
    nyquist = length // 2
    inner = 24 if block_size % 24 == 0 else next(n for n in range(32, 0, -1) if block_size % n == 0)
    outer = block_size // inner
    coef_idx = jnp.arange(length, dtype=jnp.int32).reshape(part_count, part_size)
    wavenum = jnp.where(coef_idx <= nyquist, coef_idx, coef_idx - nyquist)

    def waves(points, coefs):
        phase_idx = points * coefs % length
        angles = phase_idx.astype(jnp.float32) * (2.0 * math.pi / length)
        return jnp.cos(angles), jnp.sin(angles)

    scales = jnp.where(
        (coef_idx == 0) | (coef_idx == nyquist), 1.0 / math.sqrt(length), math.sqrt(2.0 / length)
    )
    starts = (jnp.arange(block_count, dtype=jnp.int32) * block_size)[:, None, None]
    start_cos, start_sin = waves(starts, wavenum[None])
    is_cos = (coef_idx <= nyquist)[None]
    first = jnp.where(is_cos, start_cos, start_sin) * scales
    second = jnp.where(is_cos, -start_sin, start_cos) * scales
    coarse = jnp.stack([first, second], axis=2)
    high = (jnp.arange(outer, dtype=jnp.int32) * inner)[None, :, None, None]
    low = jnp.arange(inner, dtype=jnp.int32)[None, None, :, None]
    pieces = waves(high, wavenum[:, None, None, :]) + waves(low, wavenum[:, None, None, :])
    high_cos, high_sin, low_cos, low_sin = lax.optimization_barrier(pieces)
    fine = jnp.stack([high_cos * low_cos - high_sin * low_sin, high_sin * low_cos + high_cos * low_sin])
    return coarse, fine.reshape(2, part_count, block_size, part_size)


def lat_basis(length):
    grid_idx = jnp.arange(length, dtype=jnp.int32)[:, None]
    mode_idx = jnp.arange(length, dtype=jnp.int32)[None, :]
    phase_idx = mode_idx * (2 * grid_idx + 1) % (4 * length)
    angles = phase_idx.astype(jnp.float32) * (math.pi / (2.0 * length))
    scales = jnp.where(mode_idx == 0, 1.0 / math.sqrt(length), math.sqrt(2.0 / length))
    return (jnp.cos(angles) * scales).astype(jnp.bfloat16)


def fused_kernel(
    lat_size, lon_size, own, obs_rows,
    anom, taper, level, column, row, value, coarse, fine, modes, out,
    fields, table_fwd, table_inv, fine_near, modes_near, taper_near, taper_all, hits, innov_own, innov_all,
    weighted, inverse, total, partner_part, lat_send, lat_recv, lon_send, lon_recv,
    field_ss, field_rs, local_sem, table_sem, taper_ss, taper_rs, innov_ss, innov_rs,
    gather_ss, gather_rs, mem_sem, lat_ss, lat_rs, lon_ss, lon_rs, pair_sem,
):
    lat, lon, mem = lax.axis_index("lat"), lax.axis_index("lon"), lax.axis_index("mem")
    place_count = lat_size * lon_size
    half = lon_size // 2
    me = lat * lon_size + lon
    col_count, row_count = fields.shape[3:]
    f32, bf16 = jnp.float32, jnp.bfloat16

    def device(lat_idx, lon_idx, mem_idx):
        return {"lat": lat_idx, "lon": lon_idx, "mem": mem_idx}

    def place(offset):
        spot = lax.rem(me + offset, place_count)
        return lax.div(spot, lon_size), lax.rem(spot, lon_size)

    def remote(src, dst, send, recv, target):
        return pltpu.make_async_remote_copy(
            src_ref=src, dst_ref=dst, send_sem=send, recv_sem=recv,
            device_id=target, device_id_type=pl.DeviceIdType.MESH,
        )

    barrier = pltpu.get_barrier_semaphore()

    @pl.loop(1, place_count)
    def _(offset):
        lat_idx, lon_idx = place(offset)
        pl.semaphore_signal(
            barrier, inc=1, device_id=device(lat_idx, lon_idx, mem),
            device_id_type=pl.DeviceIdType.MESH,
        )

    pl.semaphore_signal(
        barrier, inc=1, device_id=device(lat, lon, 1 - mem),
        device_id_type=pl.DeviceIdType.MESH,
    )
    pl.semaphore_wait(barrier, place_count)

    def field_copy(turn, offset):
        lat_idx, lon_idx = place(offset)
        return remote(
            anom.at[lat_idx * own + turn, lon_idx], fields.at[turn, lat, lon],
            field_ss.at[turn, offset], field_rs.at[turn, offset], device(lat_idx, lon_idx, mem),
        )

    def send_fields(turn):
        @pl.loop(1, place_count)
        def _(offset):
            field_copy(turn, offset).start()

    def own_copy(turn):
        return pltpu.make_async_copy(
            anom.at[lat * own + turn, lon], fields.at[turn, lat, lon], local_sem.at[turn]
        )

    send_fields(0)
    taper_copies = [
        remote(
            taper_all.at[lat], taper_all.at[lat], taper_ss.at[step], taper_rs.at[step],
            device(lax.rem(lat + step, lat_size), lon, mem),
        )
        for step in range(1, lat_size)
    ]
    table_copies = [
        pltpu.make_async_copy(src, dst, table_sem.at[idx])
        for idx, (src, dst) in enumerate([
            (taper.at[0], taper_near), (fine, fine_near), (modes, modes_near),
        ])
    ]
    for copy in table_copies:
        copy.start()
    for turn in range(own):
        own_copy(turn).start()

    hits[...] = jnp.zeros_like(hits)
    col_start, row_start = lon * col_count, lat * row_count
    group = 4

    @pl.loop(0, obs_rows // group)
    def _(step):
        def wide(ref):
            return jnp.concatenate([ref[pl.ds(step * group + part, 1), :] for part in range(group)], axis=1)

        keys = wide(level) * col_count + (wide(column) - col_start)
        local_row = wide(row) - row_start
        amount = wide(value)
        width = keys.shape[1]
        high = amount.astype(bf16).astype(f32)
        low = amount - high
        row_hot = lax.broadcasted_iota(jnp.int32, (row_count, width), 0) == local_row
        right = jnp.concatenate(
            [jnp.where(row_hot, high, 0.0).astype(bf16), jnp.where(row_hot, low, 0.0).astype(bf16)], axis=0
        )
        cells = lax.broadcasted_iota(jnp.int32, (col_count, width), 0)
        for lev in range(lon_size):
            left = jnp.where(cells == keys - lev * col_count, 1.0, 0.0).astype(bf16)
            hits[lev] += lax.dot_general(
                left, right, (((1,), (1,)), ((), ())), preferred_element_type=f32
            )

    for lev in range(lon_size):
        innov_own[lev] = (hits[lev, :, :row_count] + hits[lev, :, row_count:]).astype(bf16)
    innov_copies = [
        remote(
            innov_own.at[lax.rem(lon + step, lon_size)], innov_all.at[lat, lon],
            innov_ss.at[step], innov_rs.at[step], device(lat, lax.rem(lon + step, lon_size), mem),
        )
        for step in range(1, lon_size)
    ]
    for copy in innov_copies:
        copy.start()
    innov_local = pltpu.make_async_copy(innov_own.at[lon], innov_all.at[lat, lon], innov_ss.at[0])
    innov_local.start()
    table_copies[0].wait()
    taper_all[lat] = taper_near[...].astype(bf16)
    for copy in taper_copies:
        copy.start()
    send_fields(1)
    for copy in table_copies[1:]:
        copy.wait()

    @pl.loop(0, lon_size)
    def _(block):
        for part in range(lat_size):
            table = (
                coarse[block, part, 0:1, :] * fine_near[0, part]
                + coarse[block, part, 1:2, :] * fine_near[1, part]
            )
            table_inv[block, part] = table.astype(bf16)
            table_fwd[block, part] = table.T.astype(bf16)

    innov_local.wait()
    for copy in innov_copies:
        copy.wait_recv()
    gather_copies = [
        remote(
            innov_all.at[lat], innov_all.at[lat], gather_ss.at[step], gather_rs.at[step],
            device(lax.rem(lat + step, lat_size), lon, mem),
        )
        for step in range(1, lat_size)
    ]
    for copy in gather_copies:
        copy.start()
    for turn in range(2, own):
        send_fields(turn)
    total[...] = jnp.zeros_like(total)
    for copy in taper_copies + gather_copies:
        copy.wait_recv()

    mem_copy = remote(
        total.at[pl.ds((1 - mem) * half, half)], partner_part, mem_sem.at[0], mem_sem.at[1],
        device(lat, lon, 1 - mem),
    )

    @pl.loop(0, own)
    def _(turn):
        def weigh(band, block):
            product = fields[turn, band, block].astype(f32) * innov_all[band, block].astype(f32)
            lanes = pl.ds(pl.multiple_of(band * row_count, row_count), row_count)
            weighted[block, :, lanes] = product.astype(bf16)

        own_copy(turn).wait()
        weigh(lat, lon)

        @pl.loop(1, place_count)
        def _(offset):
            field_copy(turn, offset).wait_recv()
            weigh(*place(place_count - offset))

        @pl.loop(0, lat_size)
        def _(part):
            zonal = jnp.dot(table_fwd[0, part], weighted[0], preferred_element_type=f32)
            for block in range(1, lon_size):
                zonal += jnp.dot(table_fwd[block, part], weighted[block], preferred_element_type=f32)
            spectrum = jnp.dot(zonal.astype(bf16), modes_near[...], preferred_element_type=f32)
            tapered = (spectrum * taper_all[part].astype(f32)).astype(bf16)
            inverse[part] = lax.dot_general(
                tapered, modes_near[...], (((1,), (1,)), ((), ())), preferred_element_type=f32
            ).astype(bf16)

        def localize(step):
            block = lax.rem((1 - mem) * half + step, lon_size)
            localized = jnp.dot(table_inv[block, 0], inverse[0], preferred_element_type=f32)
            for part in range(1, lat_size):
                localized += jnp.dot(table_inv[block, part], inverse[part], preferred_element_type=f32)
            for band in range(lat_size):
                total[block, band] += (
                    fields[turn, band, block].astype(f32)
                    * localized[:, band * row_count:(band + 1) * row_count]
                )

        pl.loop(0, half)(localize)
        pl.when(turn == own - 1)(lambda: mem_copy.start())
        pl.loop(half, lon_size)(localize)

    mem_copy.wait_recv()
    lat_copies = [
        [
            remote(
                lat_send.at[block, lax.rem(lat + step, lat_size)], lat_recv.at[block, step],
                lat_ss.at[block, step], lat_rs.at[block, step],
                device(lax.rem(lat + step, lat_size), lon, mem),
            )
            for step in range(1, lat_size)
        ]
        for block in range(half)
    ]
    for block in range(half):
        for band in range(lat_size):
            lat_send[block, band] = (total[mem * half + block, band] + partner_part[block, band]).astype(bf16)
        for copy in lat_copies[block]:
            copy.start()

    def lon_copy(block):
        return remote(
            lon_send.at[block], lon_recv.at[lon], lon_ss.at[block], lon_rs.at[lon],
            device(lat, mem * half + block, mem),
        )

    def lon_local(block):
        return pltpu.make_async_copy(lon_send.at[block], lon_recv.at[lon], lon_ss.at[block])

    for block in range(half):
        for copy in lat_copies[block]:
            copy.wait_recv()
        summed = lat_send[block, lat].astype(f32)
        for step in range(1, lat_size):
            summed += lat_recv[block, step].astype(f32)
        lon_send[block] = summed.astype(bf16)
        pl.when(mem * half + block != lon)(lambda block=block: lon_copy(block).start())
        pl.when(mem * half + block == lon)(lambda block=block: lon_local(block).start())
    receives = lax.div(lon, half) == mem
    pair_copy = remote(lon_recv, lon_recv, pair_sem.at[0], pair_sem.at[1], device(lat, lon, 1 - mem))

    @pl.when(receives)
    def _():
        for step in range(1, lon_size):
            sender = lax.rem(lon + step, lon_size)
            remote(
                lon_send.at[0], lon_recv.at[sender], lon_ss.at[0], lon_rs.at[sender],
                device(lat, sender, mem),
            ).wait_recv()

    for block in range(half):
        pl.when(mem * half + block != lon)(lambda block=block: lon_copy(block).wait_send())
        pl.when(mem * half + block == lon)(lambda block=block: lon_local(block).wait())

    @pl.when(receives)
    def _():
        pair_copy.start()
        pair_copy.wait_send()

    @pl.when(jnp.logical_not(receives))
    def _():
        pair_copy.wait_recv()

    out[...] = lon_recv[...]
    mem_copy.wait_send()
    for copy in taper_copies + innov_copies + gather_copies + sum(lat_copies, []):
        copy.wait_send()

    @pl.loop(0, own)
    def _(turn):
        @pl.loop(1, place_count)
        def _(offset):
            field_copy(turn, offset).wait_send()


def local(anomalies, taper, obs_row, obs_col, obs_level, obs_value):
    member_count, level_count, col_count, row_count = anomalies.shape
    lon_size, lat_size = lax.axis_size("lon"), lax.axis_size("lat")
    lon_total, lat_total = col_count * lon_size, row_count * lat_size
    ensemble = member_count * lax.axis_size("mem")
    own = member_count // lat_size
    place_count = lat_size * lon_size
    half = lon_size // 2
    part_count = taper.shape[1]
    coarse, fine = lon_factors(lon_size, col_count, lat_size, part_count)
    lat_table = lat_basis(lat_total)
    f32, bf16 = jnp.float32, jnp.bfloat16
    slab = (col_count, row_count)
    whole = pl.BlockSpec(memory_space=pl.ANY)
    near = pl.BlockSpec(memory_space=pltpu.VMEM)
    dma = pltpu.SemaphoreType.DMA
    result = pl.pallas_call(
        functools.partial(fused_kernel, lat_size, lon_size, own, obs_row.shape[0]),
        out_shape=jax.ShapeDtypeStruct((level_count,) + slab, bf16),
        in_specs=[whole, whole, near, near, near, near, near, whole, whole],
        out_specs=near,
        scratch_shapes=[
            pltpu.VMEM((own, lat_size, lon_size) + slab, bf16),
            pltpu.VMEM((lon_size, lat_size, part_count, col_count), bf16),
            pltpu.VMEM((lon_size, lat_size, col_count, part_count), bf16),
            pltpu.VMEM((2, lat_size, col_count, part_count), f32),
            pltpu.VMEM((lat_total, lat_total), bf16),
            pltpu.VMEM((part_count, lat_total), f32),
            pltpu.VMEM((lat_size, part_count, lat_total), bf16),
            pltpu.VMEM((level_count, col_count, 2 * row_count), f32),
            pltpu.VMEM((level_count,) + slab, bf16),
            pltpu.VMEM((lat_size, lon_size) + slab, bf16),
            pltpu.VMEM((lon_size, col_count, lat_total), bf16),
            pltpu.VMEM((lat_size, part_count, lat_total), bf16),
            pltpu.VMEM((lon_size, lat_size) + slab, f32),
            pltpu.VMEM((half, lat_size) + slab, f32),
            pltpu.VMEM((half, lat_size) + slab, bf16),
            pltpu.VMEM((half, lat_size) + slab, bf16),
            pltpu.VMEM((half,) + slab, bf16),
            pltpu.VMEM((level_count,) + slab, bf16),
            dma((own, place_count)), dma((own, place_count)), dma((own,)), dma((3,)),
            dma((lat_size,)), dma((lat_size,)), dma((lon_size,)), dma((lon_size,)),
            dma((lat_size,)), dma((lat_size,)), dma((2,)), dma((half, lat_size)), dma((half, lat_size)),
            dma((half,)), dma((lon_size,)), dma((2,)),
        ],
        compiler_params=pltpu.CompilerParams(
            collective_id=0, has_side_effects=True, vmem_limit_bytes=60 * 1024 * 1024
        ),
    )(
        anomalies, taper, obs_level, obs_col, obs_row, obs_value, coarse, fine, lat_table,
    )
    return result.astype(f32) / (ensemble - 1)


def solution(mesh):
    in_specs = (
        P("mem", None, "lon", "lat"),
        P("lon", "lat", None),
        P("lat", "lon"),
        P("lat", "lon"),
        P("lat", "lon"),
        P("lat", "lon"),
    )
    out_specs = P(None, "lon", "lat")
    return jax.shard_map(local, mesh=mesh, in_specs=in_specs, out_specs=out_specs, check_vma=False)
```

```python
import functools
import math

import jax
import jax.numpy as jnp
from jax import lax
from jax.experimental import pallas as pl
from jax.experimental.pallas import tpu as pltpu
from jax.sharding import PartitionSpec as P


def lon_factors(block_count, block_size, part_count, part_size):
    length = block_count * block_size
    nyquist = length // 2
    inner = 24 if block_size % 24 == 0 else next(n for n in range(32, 0, -1) if block_size % n == 0)
    outer = block_size // inner
    coef_idx = jnp.arange(length, dtype=jnp.int32).reshape(part_count, part_size)
    wavenum = jnp.where(coef_idx <= nyquist, coef_idx, coef_idx - nyquist)

    def waves(points, coefs):
        phase_idx = points * coefs % length
        angles = phase_idx.astype(jnp.float32) * (2.0 * math.pi / length)
        return jnp.cos(angles), jnp.sin(angles)

    scales = jnp.where(
        (coef_idx == 0) | (coef_idx == nyquist), 1.0 / math.sqrt(length), math.sqrt(2.0 / length)
    )
    starts = (jnp.arange(block_count, dtype=jnp.int32) * block_size)[:, None, None]
    start_cos, start_sin = waves(starts, wavenum[None])
    is_cos = (coef_idx <= nyquist)[None]
    first = jnp.where(is_cos, start_cos, start_sin) * scales
    second = jnp.where(is_cos, -start_sin, start_cos) * scales
    coarse = jnp.stack([first, second], axis=2)
    high = (jnp.arange(outer, dtype=jnp.int32) * inner)[None, :, None, None]
    low = jnp.arange(inner, dtype=jnp.int32)[None, None, :, None]
    pieces = waves(high, wavenum[:, None, None, :]) + waves(low, wavenum[:, None, None, :])
    high_cos, high_sin, low_cos, low_sin = lax.optimization_barrier(pieces)
    fine = jnp.stack([high_cos * low_cos - high_sin * low_sin, high_sin * low_cos + high_cos * low_sin])
    return coarse, fine.reshape(2, part_count, block_size, part_size)


def lat_basis(length):
    inner = next(size for size in range(32, 0, -1) if length % size == 0)
    outer = length // inner
    mode_idx = jnp.arange(length, dtype=jnp.int32)[None, :]

    def waves(points):
        phase_idx = mode_idx * points[:, None] % (4 * length)
        angles = phase_idx.astype(jnp.float32) * (math.pi / (2.0 * length))
        return jnp.cos(angles), jnp.sin(angles)

    scales = jnp.where(mode_idx == 0, 1.0 / math.sqrt(length), math.sqrt(2.0 / length))
    high_cos, high_sin = waves(jnp.arange(outer, dtype=jnp.int32) * (2 * inner))
    low_cos, low_sin = waves(jnp.arange(inner, dtype=jnp.int32) * 2 + 1)
    high_cos, high_sin, low_cos, low_sin = lax.optimization_barrier(
        (high_cos * scales, high_sin * scales, low_cos, low_sin)
    )
    basis = high_cos[:, None, :] * low_cos[None] - high_sin[:, None, :] * low_sin[None]
    return basis.reshape(length, length).astype(jnp.bfloat16)


def fused_kernel(
    lat_size, lon_size, own, obs_rows,
    anom, taper, level, column, row, value, coarse, fine, modes, out,
    fields, table_fwd, table_inv, fine_near, modes_near, taper_near, taper_all, hits, innov_own, innov_all,
    weighted, inverse, total, partner_part, lat_send, lat_recv, lon_send, lon_recv,
    field_ss, field_rs, local_sem, table_sem, taper_ss, taper_rs, innov_ss, innov_rs,
    gather_ss, gather_rs, mem_sem, lat_ss, lat_rs, lon_ss, lon_rs, pair_sem,
):
    lat, lon, mem = lax.axis_index("lat"), lax.axis_index("lon"), lax.axis_index("mem")
    place_count = lat_size * lon_size
    half = lon_size // 2
    me = lat * lon_size + lon
    col_count, row_count = fields.shape[3:]
    f32, bf16 = jnp.float32, jnp.bfloat16

    def device(lat_idx, lon_idx, mem_idx):
        return {"lat": lat_idx, "lon": lon_idx, "mem": mem_idx}

    def place(offset):
        spot = lax.rem(me + offset, place_count)
        return lax.div(spot, lon_size), lax.rem(spot, lon_size)

    def remote(src, dst, send, recv, target):
        return pltpu.make_async_remote_copy(
            src_ref=src, dst_ref=dst, send_sem=send, recv_sem=recv,
            device_id=target, device_id_type=pl.DeviceIdType.MESH,
        )

    barrier = pltpu.get_barrier_semaphore()

    @pl.loop(1, place_count)
    def _(offset):
        lat_idx, lon_idx = place(offset)
        pl.semaphore_signal(
            barrier, inc=1, device_id=device(lat_idx, lon_idx, mem),
            device_id_type=pl.DeviceIdType.MESH,
        )

    pl.semaphore_signal(
        barrier, inc=1, device_id=device(lat, lon, 1 - mem),
        device_id_type=pl.DeviceIdType.MESH,
    )
    pl.semaphore_wait(barrier, place_count)

    def field_copy(turn, offset):
        lat_idx, lon_idx = place(offset)
        return remote(
            anom.at[lat_idx * own + turn, lon_idx], fields.at[turn, lat, lon],
            field_ss.at[turn, offset], field_rs.at[turn, offset], device(lat_idx, lon_idx, mem),
        )

    def send_fields(turn):
        @pl.loop(1, place_count)
        def _(offset):
            field_copy(turn, offset).start()

    def own_copy(turn):
        return pltpu.make_async_copy(
            anom.at[lat * own + turn, lon], fields.at[turn, lat, lon], local_sem.at[turn]
        )

    send_fields(0)
    taper_copies = [
        remote(
            taper_all.at[lat], taper_all.at[lat], taper_ss.at[step], taper_rs.at[step],
            device(lax.rem(lat + step, lat_size), lon, mem),
        )
        for step in range(1, lat_size)
    ]
    table_copies = [
        pltpu.make_async_copy(src, dst, table_sem.at[idx])
        for idx, (src, dst) in enumerate([
            (taper.at[0], taper_near), (fine, fine_near), (modes, modes_near),
        ])
    ]
    for copy in table_copies:
        copy.start()
    for turn in range(own):
        own_copy(turn).start()

    hits[...] = jnp.zeros_like(hits)
    col_start, row_start = lon * col_count, lat * row_count
    group = 4

    @pl.loop(0, obs_rows // group)
    def _(step):
        def wide(ref):
            return jnp.concatenate([ref[pl.ds(step * group + part, 1), :] for part in range(group)], axis=1)

        keys = wide(level) * col_count + (wide(column) - col_start)
        local_row = wide(row) - row_start
        amount = wide(value)
        width = keys.shape[1]
        high = amount.astype(bf16).astype(f32)
        low = amount - high
        row_hot = lax.broadcasted_iota(jnp.int32, (row_count, width), 0) == local_row
        right = jnp.concatenate(
            [jnp.where(row_hot, high, 0.0).astype(bf16), jnp.where(row_hot, low, 0.0).astype(bf16)], axis=0
        )
        cells = lax.broadcasted_iota(jnp.int32, (col_count, width), 0)
        for lev in range(lon_size):
            left = jnp.where(cells == keys - lev * col_count, 1.0, 0.0).astype(bf16)
            hits[lev] += lax.dot_general(
                left, right, (((1,), (1,)), ((), ())), preferred_element_type=f32
            )

    for lev in range(lon_size):
        innov_own[lev] = (hits[lev, :, :row_count] + hits[lev, :, row_count:]).astype(bf16)
    innov_copies = [
        remote(
            innov_own.at[lax.rem(lon + step, lon_size)], innov_all.at[lat, lon],
            innov_ss.at[step], innov_rs.at[step], device(lat, lax.rem(lon + step, lon_size), mem),
        )
        for step in range(1, lon_size)
    ]
    for copy in innov_copies:
        copy.start()
    innov_local = pltpu.make_async_copy(innov_own.at[lon], innov_all.at[lat, lon], innov_ss.at[0])
    innov_local.start()
    table_copies[0].wait()
    taper_all[lat] = taper_near[...].astype(bf16)
    for copy in taper_copies:
        copy.start()
    send_fields(1)
    for copy in table_copies[1:]:
        copy.wait()

    @pl.loop(0, lon_size)
    def _(block):
        for part in range(lat_size):
            table = (
                coarse[block, part, 0:1, :] * fine_near[0, part]
                + coarse[block, part, 1:2, :] * fine_near[1, part]
            )
            table_inv[block, part] = table.astype(bf16)
            table_fwd[block, part] = table.T.astype(bf16)

    innov_local.wait()
    for copy in innov_copies:
        copy.wait_recv()
    gather_copies = [
        remote(
            innov_all.at[lat], innov_all.at[lat], gather_ss.at[step], gather_rs.at[step],
            device(lax.rem(lat + step, lat_size), lon, mem),
        )
        for step in range(1, lat_size)
    ]
    for copy in gather_copies:
        copy.start()
    for turn in range(2, own):
        send_fields(turn)
    total[...] = jnp.zeros_like(total)
    for copy in taper_copies + gather_copies:
        copy.wait_recv()

    mem_copy = remote(
        total.at[pl.ds((1 - mem) * half, half)], partner_part, mem_sem.at[0], mem_sem.at[1],
        device(lat, lon, 1 - mem),
    )

    @pl.loop(0, own)
    def _(turn):
        def weigh(band, block):
            product = fields[turn, band, block].astype(f32) * innov_all[band, block].astype(f32)
            lanes = pl.ds(pl.multiple_of(band * row_count, row_count), row_count)
            weighted[block, :, lanes] = product.astype(bf16)

        own_copy(turn).wait()
        weigh(lat, lon)

        @pl.loop(1, place_count)
        def _(offset):
            field_copy(turn, offset).wait_recv()
            weigh(*place(place_count - offset))

        @pl.loop(0, lat_size)
        def _(part):
            zonal = jnp.dot(table_fwd[0, part], weighted[0], preferred_element_type=f32)
            for block in range(1, lon_size):
                zonal += jnp.dot(table_fwd[block, part], weighted[block], preferred_element_type=f32)
            spectrum = jnp.dot(zonal.astype(bf16), modes_near[...], preferred_element_type=f32)
            tapered = (spectrum * taper_all[part].astype(f32)).astype(bf16)
            inverse[part] = lax.dot_general(
                tapered, modes_near[...], (((1,), (1,)), ((), ())), preferred_element_type=f32
            ).astype(bf16)

        def localize(step):
            block = lax.rem((1 - mem) * half + step, lon_size)
            localized = jnp.dot(table_inv[block, 0], inverse[0], preferred_element_type=f32)
            for part in range(1, lat_size):
                localized += jnp.dot(table_inv[block, part], inverse[part], preferred_element_type=f32)
            for band in range(lat_size):
                total[block, band] += (
                    fields[turn, band, block].astype(f32)
                    * localized[:, band * row_count:(band + 1) * row_count]
                )

        pl.loop(0, half)(localize)
        pl.when(turn == own - 1)(lambda: mem_copy.start())
        pl.loop(half, lon_size)(localize)

    mem_copy.wait_recv()
    lat_copies = [
        [
            remote(
                lat_send.at[block, lax.rem(lat + step, lat_size)], lat_recv.at[block, step],
                lat_ss.at[block, step], lat_rs.at[block, step],
                device(lax.rem(lat + step, lat_size), lon, mem),
            )
            for step in range(1, lat_size)
        ]
        for block in range(half)
    ]
    for block in range(half):
        for band in range(lat_size):
            lat_send[block, band] = (total[mem * half + block, band] + partner_part[block, band]).astype(bf16)
        for copy in lat_copies[block]:
            copy.start()

    def lon_copy(block):
        return remote(
            lon_send.at[block], lon_recv.at[lon], lon_ss.at[block], lon_rs.at[lon],
            device(lat, mem * half + block, mem),
        )

    def lon_local(block):
        return pltpu.make_async_copy(lon_send.at[block], lon_recv.at[lon], lon_ss.at[block])

    for block in range(half):
        for copy in lat_copies[block]:
            copy.wait_recv()
        summed = lat_send[block, lat].astype(f32)
        for step in range(1, lat_size):
            summed += lat_recv[block, step].astype(f32)
        lon_send[block] = summed.astype(bf16)
        pl.when(mem * half + block != lon)(lambda block=block: lon_copy(block).start())
        pl.when(mem * half + block == lon)(lambda block=block: lon_local(block).start())
    receives = lax.div(lon, half) == mem
    pair_copy = remote(lon_recv, lon_recv, pair_sem.at[0], pair_sem.at[1], device(lat, lon, 1 - mem))

    @pl.when(receives)
    def _():
        for step in range(1, lon_size):
            sender = lax.rem(lon + step, lon_size)
            remote(
                lon_send.at[0], lon_recv.at[sender], lon_ss.at[0], lon_rs.at[sender],
                device(lat, sender, mem),
            ).wait_recv()

    for block in range(half):
        pl.when(mem * half + block != lon)(lambda block=block: lon_copy(block).wait_send())
        pl.when(mem * half + block == lon)(lambda block=block: lon_local(block).wait())

    @pl.when(receives)
    def _():
        pair_copy.start()
        pair_copy.wait_send()

    @pl.when(jnp.logical_not(receives))
    def _():
        pair_copy.wait_recv()

    out[...] = lon_recv[...]
    mem_copy.wait_send()
    for copy in taper_copies + innov_copies + gather_copies + sum(lat_copies, []):
        copy.wait_send()

    @pl.loop(0, own)
    def _(turn):
        @pl.loop(1, place_count)
        def _(offset):
            field_copy(turn, offset).wait_send()


def local(anomalies, taper, obs_row, obs_col, obs_level, obs_value):
    member_count, level_count, col_count, row_count = anomalies.shape
    lon_size, lat_size = lax.axis_size("lon"), lax.axis_size("lat")
    lon_total, lat_total = col_count * lon_size, row_count * lat_size
    ensemble = member_count * lax.axis_size("mem")
    own = member_count // lat_size
    place_count = lat_size * lon_size
    half = lon_size // 2
    part_count = taper.shape[1]
    coarse, fine = lon_factors(lon_size, col_count, lat_size, part_count)
    lat_table = lat_basis(lat_total)
    f32, bf16 = jnp.float32, jnp.bfloat16
    slab = (col_count, row_count)
    whole = pl.BlockSpec(memory_space=pl.ANY)
    near = pl.BlockSpec(memory_space=pltpu.VMEM)
    dma = pltpu.SemaphoreType.DMA
    result = pl.pallas_call(
        functools.partial(fused_kernel, lat_size, lon_size, own, obs_row.shape[0]),
        out_shape=jax.ShapeDtypeStruct((level_count,) + slab, bf16),
        in_specs=[whole, whole, near, near, near, near, near, whole, whole],
        out_specs=near,
        scratch_shapes=[
            pltpu.VMEM((own, lat_size, lon_size) + slab, bf16),
            pltpu.VMEM((lon_size, lat_size, part_count, col_count), bf16),
            pltpu.VMEM((lon_size, lat_size, col_count, part_count), bf16),
            pltpu.VMEM((2, lat_size, col_count, part_count), f32),
            pltpu.VMEM((lat_total, lat_total), bf16),
            pltpu.VMEM((part_count, lat_total), f32),
            pltpu.VMEM((lat_size, part_count, lat_total), bf16),
            pltpu.VMEM((level_count, col_count, 2 * row_count), f32),
            pltpu.VMEM((level_count,) + slab, bf16),
            pltpu.VMEM((lat_size, lon_size) + slab, bf16),
            pltpu.VMEM((lon_size, col_count, lat_total), bf16),
            pltpu.VMEM((lat_size, part_count, lat_total), bf16),
            pltpu.VMEM((lon_size, lat_size) + slab, f32),
            pltpu.VMEM((half, lat_size) + slab, f32),
            pltpu.VMEM((half, lat_size) + slab, bf16),
            pltpu.VMEM((half, lat_size) + slab, bf16),
            pltpu.VMEM((half,) + slab, bf16),
            pltpu.VMEM((level_count,) + slab, bf16),
            dma((own, place_count)), dma((own, place_count)), dma((own,)), dma((3,)),
            dma((lat_size,)), dma((lat_size,)), dma((lon_size,)), dma((lon_size,)),
            dma((lat_size,)), dma((lat_size,)), dma((2,)), dma((half, lat_size)), dma((half, lat_size)),
            dma((half,)), dma((lon_size,)), dma((2,)),
        ],
        compiler_params=pltpu.CompilerParams(
            collective_id=0, has_side_effects=True, vmem_limit_bytes=60 * 1024 * 1024
        ),
    )(
        anomalies, taper, obs_level, obs_col, obs_row, obs_value, coarse, fine, lat_table,
    )
    return result.astype(f32) / (ensemble - 1)


def solution(mesh):
    in_specs = (
        P("mem", None, "lon", "lat"),
        P("lon", "lat", None),
        P("lat", "lon"),
        P("lat", "lon"),
        P("lat", "lon"),
        P("lat", "lon"),
    )
    out_specs = P(None, "lon", "lat")
    return jax.shard_map(local, mesh=mesh, in_specs=in_specs, out_specs=out_specs, check_vma=False)
```
